32 devices in a mesh: rep: 1, dp: 32 (over x, y, z, core).
Axes of the slice: x: 2, y: 2, z: 4, core: 2. Of those that a mesh axis runs over, the one named last changes fastest.
Arguments:
- x: bfloat16 [32, 2048, 640], P(('rep', 'dp'))
- dy: bfloat16 [32, 2048, 640], P(('rep', 'dp'))
- w_gate: bfloat16 [2, 640, 2560], replicated
- w_up: bfloat16 [2, 640, 2560], replicated
- w_down: bfloat16 [2, 2560, 640], replicated
- m_w_gate: float32 [2, 640, 2560], P(None, 'dp')
- m_w_up: float32 [2, 640, 2560], P(None, 'dp')
- m_w_down: float32 [2, 2560, 640], P(None, 'dp')
- v_w_gate: float32 [2, 640, 2560], P(None, 'dp')
- v_w_up: float32 [2, 640, 2560], P(None, 'dp')
- v_w_down: float32 [2, 2560, 640], P(None, 'dp')
Outputs:
- output 1: bfloat16 [2, 640, 2560], P('rep')
- output 2: bfloat16 [2, 640, 2560], P('rep')
- output 3: bfloat16 [2, 2560, 640], P('rep')
- output 4: float32 [2, 640, 2560], P('rep', 'dp')
- output 5: float32 [2, 640, 2560], P('rep', 'dp')
- output 6: float32 [2, 2560, 640], P('rep', 'dp')
- output 7: float32 [2, 640, 2560], P('rep', 'dp')
- output 8: float32 [2, 640, 2560], P('rep', 'dp')
- output 9: float32 [2, 2560, 640], P('rep', 'dp')
All inputs are finite; a program needn't handle non-finite values.
Results may differ from the reference program's by a relative error of at most 0.022.
Values are sent between devices in bfloat16 or wider.
A program may use at most 2 GiB of HBM per device.

```python
import jax
import jax.numpy as jnp
from jax import lax

SEQUENCES = 32
TOKENS = 2048
D = 640
FF = 2560
LAYERS = 2
NAMES = ("w_gate", "w_up", "w_down")
SHAPES = {"w_gate": (LAYERS, D, FF), "w_up": (LAYERS, D, FF), "w_down": (LAYERS, FF, D)}


def bump(key, n, height):
    away = (jnp.arange(n, dtype=jnp.int32) - jax.random.randint(key, (), 0, n, jnp.int32)) % n
    return jnp.where(away < n // 8, height, 1.0)


def together(key, own, strength):
    shared = jax.random.normal(key, own.shape[1:], jnp.float32)
    return (own + strength * shared) * lax.rsqrt(1 + strength * strength)


def setup_inputs(seed: int = 0, part: int = 0) -> dict:
    kx, kdy, ka, kb, kz, kf, kh, kl, *keys = jax.random.split(jax.random.key(seed), 8 + 3 * len(NAMES))
    kx, kdy, ka, kb = (jax.random.fold_in(k, part) for k in (kx, kdy, ka, kb))
    kw, km, kv = (keys[i::3] for i in range(3))
    shape = (SEQUENCES, TOKENS, D)
    much_x, much_dy = jax.random.uniform(kz, (2,), jnp.float32, 0.0, 1.0)
    loud = 2.0 ** jax.random.uniform(jax.random.fold_in(kz, 1), (), jnp.float32, -1.0, 2.0)
    layers = 2.0 ** jax.random.uniform(kl, (LAYERS, 1, 1), jnp.float32, -1.0, 1.0)
    x = together(ka, jax.random.normal(kx, shape, jnp.float32), much_x) * bump(kf, D, 4.0)
    dy = together(kb, jax.random.normal(kdy, shape, jnp.float32), much_dy)
    drawn = {"x": x.astype(jnp.bfloat16), "dy": (loud * dy * (SEQUENCES * TOKENS) ** -0.5).astype(jnp.bfloat16)}
    for key, name in zip(kw, NAMES, strict=True):
        w = jax.random.normal(key, SHAPES[name], jnp.float32) * SHAPES[name][1] ** -0.5
        drawn[name] = (w * {"w_gate": 1.0, "w_up": bump(kh, FF, 4.0), "w_down": layers}[name]).astype(jnp.bfloat16)
    for key, name in zip(km, NAMES, strict=True):
        drawn[f"m_{name}"] = 0.1 * jax.random.normal(key, SHAPES[name], jnp.float32)
    for key, name in zip(kv, NAMES, strict=True):
        drawn[f"v_{name}"] = jax.random.uniform(key, SHAPES[name], jnp.float32, 0.005, 0.015)
    return drawn


def matmul(a, w):
    return jnp.dot(a, w, preferred_element_type=jnp.float32).astype(jnp.bfloat16)


def normed(h):
    wide = h.astype(jnp.float32)
    scale = lax.rsqrt(jnp.mean(wide**2, -1, keepdims=True) + 1e-6)
    return (wide * scale).astype(jnp.bfloat16)


def layer(h, w):
    a = normed(h)
    gate = jnp.dot(a, w["w_gate"], preferred_element_type=jnp.float32)
    up = jnp.dot(a, w["w_up"], preferred_element_type=jnp.float32)
    return h + matmul((jax.nn.silu(gate) * up).astype(jnp.bfloat16), w["w_down"])


def adamw(w, m, v, g):
    m = 0.9 * m + 0.1 * g
    v = 0.95 * v + 0.05 * g * g
    step = m * lax.rsqrt(v + 1e-8) + 0.1 * w
    return (w - 0.02 * step).astype(jnp.bfloat16), m, v


def clipped(gradients, sum_of_squares, count):
    factor = jnp.minimum(1.0, 0.5 * lax.rsqrt(sum_of_squares / count + 1e-30))
    return [g * factor for g in gradients]


def stack(weights, h):
    return lax.scan(lambda h, w: (layer(h, w), None), h, weights)[0]


def reference(x, dy, w_gate, w_up, w_down, m_w_gate, m_w_up, m_w_down, v_w_gate, v_w_up, v_w_down):
    weights = dict(zip(NAMES, (w_gate, w_up, w_down), strict=True))

    def take(so_far, sequence):
        h, by_y = sequence
        _, back = jax.vjp(lambda w: stack(w, h), weights)
        return jax.tree.map(lambda total, term: total + term.astype(jnp.float32), so_far, back(by_y)[0]), None

    none_yet = {name: jnp.zeros(w.shape, jnp.float32) for name, w in weights.items()}
    by_weights, _ = lax.scan(take, none_yet, (x, dy))
    gradients = [by_weights[name].astype(jnp.bfloat16).astype(jnp.float32) for name in NAMES]
    gradients = clipped(gradients, sum(jnp.sum(g * g) for g in gradients), sum(g.size for g in gradients))
    new = [
        adamw(w.astype(jnp.float32), m, v, g)
        for w, m, v, g in zip((w_gate, w_up, w_down), (m_w_gate, m_w_up, m_w_down), (v_w_gate, v_w_up, v_w_down), gradients, strict=True)
    ]
    return tuple(one[which] for which in range(3) for one in new)
```

```python
import jax
import jax.numpy as jnp
from jax import lax
from jax.sharding import PartitionSpec as P

F32, BF16 = jnp.float32, jnp.bfloat16
COUNT = 6 * 640 * 2560


def dot(a, b, ca, cb):
    return lax.dot_general(a, b, (((ca,), (cb,)), ((), ())), preferred_element_type=F32)


def norm_scale(h):
    wide = h.astype(F32)
    return wide, lax.rsqrt(jnp.mean(wide**2, -1, keepdims=True) + 1e-6)


def hidden(a, wg, wu):
    gate, up = dot(a, wg, 1, 0), dot(a, wu, 1, 0)
    return gate, up, (jax.nn.silu(gate) * up).astype(BF16)


def hidden_back(ds, gate, up):
    ds = ds.astype(F32)
    sig = jax.nn.sigmoid(gate)
    d_up = (ds * (gate * sig)).astype(BF16)
    d_gate = (ds * up * (sig * (1 + gate * (1 - sig)))).astype(BF16)
    return d_gate, d_up


def gradients(x, dy, wg, wu, wd):
    wide0, r0 = norm_scale(x)
    a1 = (wide0 * r0).astype(BF16)
    gate1, up1, s1 = hidden(a1, wg[0], wu[0])
    h1 = x + dot(s1, wd[0], 1, 0).astype(BF16)
    wide1, r1 = norm_scale(h1)
    a2 = (wide1 * r1).astype(BF16)
    gate2, up2, s2 = hidden(a2, wg[1], wu[1])

    ds2 = dot(dy, wd[1], 1, 1).astype(BF16)
    d_gate2, d_up2 = hidden_back(ds2, gate2, up2)
    da2 = (dot(d_gate2, wg[1], 1, 1).astype(BF16) + dot(d_up2, wu[1], 1, 1).astype(BF16)).astype(F32)
    back = da2 * r1 - wide1 * (r1**3 * jnp.mean(da2 * wide1, -1, keepdims=True))
    dh1 = dy + back.astype(BF16)
    ds1 = dot(dh1, wd[0], 1, 1).astype(BF16)
    d_gate1, d_up1 = hidden_back(ds1, gate1, up1)

    terms = ((a1, d_gate1), (a1, d_up1), (s1, dh1)), ((a2, d_gate2), (a2, d_up2), (s2, dy))
    return [[dot(a, b, 0, 0).astype(BF16) for a, b in layer] for layer in terms]


def adamw(w, m, v, g):
    m = 0.9 * m + 0.1 * g
    v = 0.95 * v + 0.05 * g * g
    step = m * lax.rsqrt(v + 1e-8) + 0.1 * w
    return (w - 0.02 * step).astype(BF16), m, v


def solution(mesh):
    n = mesh.shape["dp"]

    def body(x, dy, *arrays):
        w, m, v = (arrays[i : i + 3] for i in (0, 3, 6))
        me = lax.axis_index("dp")
        terms = gradients(x[0], dy[0], *w)
        summed = [[None] * 3 for _ in range(2)]
        for layer in (1, 0):
            for which in (2, 0, 1):
                term = terms[layer][which]
                rows, columns = term.shape
                flat = lax.psum_scatter(term.reshape(n * 400, 128), "dp", scatter_dimension=0, tiled=True)
                summed[layer][which] = flat.reshape(rows // n, columns)
        g = [jnp.stack([summed[layer][which] for layer in range(2)]).astype(F32) for which in range(3)]
        total = lax.psum(sum(jnp.sum(t * t) for t in g), "dp")
        factor = jnp.minimum(1.0, 0.5 * lax.rsqrt(total / COUNT + 1e-30))
        new = []
        for which in range(3):
            rows = w[which].shape[1] // n
            mine = lax.dynamic_slice_in_dim(w[which], me * rows, rows, 1).astype(F32)
            new.append(adamw(mine, m[which], v[which], g[which] * factor))
        weights = [lax.all_gather(one[0], "dp", axis=1, tiled=True) for one in new]
        return (*weights, *(one[1] for one in new), *(one[2] for one in new))

    moments = P(None, "dp", None)
    return jax.shard_map(
        body,
        mesh=mesh,
        in_specs=(P(("rep", "dp")), P(("rep", "dp")), *[P()] * 3, *[moments] * 6),
        out_specs=(*[P("rep")] * 3, *[P("rep", "dp")] * 6),
        check_vma=False,
    )
```

```python
import functools

import jax
import jax.numpy as jnp
from jax import lax
from jax.experimental import pallas as pl
from jax.experimental.pallas import tpu as pltpu
from jax.sharding import PartitionSpec as P

F32, BF16 = jnp.float32, jnp.bfloat16


def dot(a, b, ca, cb):
    return lax.dot_general(a, b, (((ca,), (cb,)), ((), ())), preferred_element_type=F32)


def norm_scale(h):
    wide = h.astype(F32)
    return wide, lax.rsqrt(jnp.mean(wide**2, -1, keepdims=True) + 1e-6)


def hidden(a, wg, wu):
    gate, up = dot(a, wg, 1, 0), dot(a, wu, 1, 0)
    return gate, up, (jax.nn.silu(gate) * up).astype(BF16)


def hidden_back(ds, gate, up):
    ds = ds.astype(F32)
    sig = jax.nn.sigmoid(gate)
    d_up = (ds * (gate * sig)).astype(BF16)
    d_gate = (ds * up * (sig * (1 + gate * (1 - sig)))).astype(BF16)
    return d_gate, d_up


def gradients(x, dy, wg, wu, wd):
    wide0, r0 = norm_scale(x)
    a1 = (wide0 * r0).astype(BF16)
    gate1, up1, s1 = hidden(a1, wg[0], wu[0])
    h1 = x + dot(s1, wd[0], 1, 0).astype(BF16)
    wide1, r1 = norm_scale(h1)
    a2 = (wide1 * r1).astype(BF16)
    gate2, up2, s2 = hidden(a2, wg[1], wu[1])

    ds2 = dot(dy, wd[1], 1, 1).astype(BF16)
    d_gate2, d_up2 = hidden_back(ds2, gate2, up2)
    da2 = (dot(d_gate2, wg[1], 1, 1).astype(BF16) + dot(d_up2, wu[1], 1, 1).astype(BF16)).astype(F32)
    back = da2 * r1 - wide1 * (r1**3 * jnp.mean(da2 * wide1, -1, keepdims=True))
    dh1 = dy + back.astype(BF16)
    ds1 = dot(dh1, wd[0], 1, 1).astype(BF16)
    d_gate1, d_up1 = hidden_back(ds1, gate1, up1)

    terms = ((a1, d_gate1), (a1, d_up1), (s1, dh1)), ((a2, d_gate2), (a2, d_up2), (s2, dy))
    return [[dot(a, b, 0, 0).astype(BF16) for a, b in layer] for layer in terms]


MESH = pl.DeviceIdType.MESH
MATRICES = (("d", 0, 1, 2), ("w", 0, 1, 0), ("w", 1, 1, 1), ("d", 1, 0, 2), ("w", 2, 0, 0), ("w", 3, 0, 1))
SIX = range(6)


def step_kernel(count, *refs):
    terms, weights, moments, out_w, out_m = refs[0:6], refs[6:9], refs[9:15], refs[15:18], refs[18:24]
    own_w, own_d, two_w, two_d, r1_w, r1_d, r2_w, r2_d, zl_w, zl_d, zr_w, zr_d = refs[24:36]
    tmp_w, tmp_d, g_w, g_d, state_w, state_d, old_w, old_d, new_w, got_w, norm = refs[36:47]
    (loc_sem, aux_sem, two_s, two_r, s1_s, s1_r, s2_s, s2_r, z_s, zl_r, zr_r, g_s, g_r, n_s, n_r, nz_r, w_s, w_r, ag_r, agz_s, ag1_s, ag2_s,
     ag3_s, agt_s, agt_r, out_s, out2_s) = refs[47:74]
    own, two = {"w": own_w, "d": own_d}, {"w": two_w, "d": two_d}
    r1, r2 = {"w": r1_w, "d": r1_d}, {"w": r2_w, "d": r2_d}
    zl, zr, tmp = {"w": zl_w, "d": zl_d}, {"w": zr_w, "d": zr_d}, {"w": tmp_w, "d": tmp_d}

    me = lax.axis_index("dp")
    core, z, y, x = lax.rem(me, 2), lax.rem(me // 2, 4), lax.rem(me // 8, 2), me // 16
    half = own_w.shape[-1]

    def device(x, y, z, core):
        return {"dp": ((x * 2 + y) * 4 + z) * 2 + core}

    partner = device(x, y, z, 1 - core)
    by_x, by_y = device(1 - x, y, z, core), device(x, 1 - y, z, core)
    right, left = device(x, y, z + 1, core), device(x, y, z - 1, core)
    line = [device(x, y, lax.rem(z + o, 4), core) for o in (1, 2, 3)]

    def columns(c):
        return pl.ds(pl.multiple_of(c * half, 128), half)

    def remote(src, dst, send, recv, to):
        return pltpu.make_async_remote_copy(src_ref=src, dst_ref=dst, send_sem=send, recv_sem=recv, device_id=to, device_id_type=MESH)

    barrier = pltpu.get_barrier_semaphore()
    for other in (partner, by_x, by_y, *line):
        pl.semaphore_signal(barrier, inc=1, device_id=other, device_id_type=MESH)
    pl.semaphore_wait(barrier, 6)

    def half_of(j, c):
        return terms[j].at[:, :, :, columns(c)] if MATRICES[j][0] == "w" else terms[j].at[:, :, c]

    def to_partner(j):
        kind, t, _, _ = MATRICES[j]
        return remote(half_of(j, 1 - core), two[kind].at[t], two_s.at[j], two_r.at[j], partner)

    def bring(j):
        kind, t, _, _ = MATRICES[j]
        return pltpu.make_async_copy(half_of(j, core), own[kind].at[t], loc_sem.at[j])

    for j in SIX:
        to_partner(j).start()
        bring(j).start()
    chip = (x * 2 + y, z)
    aux = [pltpu.make_async_copy(moments[i], (state_w, state_w, state_w, state_w, state_d, state_d)[i].at[(0, 1, 2, 3, 0, 1)[i]], aux_sem.at[i]) for i in SIX]
    aux += [pltpu.make_async_copy(weights[i].at[:, chip[0], chip[1]], old_w.at[i], aux_sem.at[6 + i]) for i in range(2)]
    aux += [pltpu.make_async_copy(weights[2].at[:, chip[0], chip[1], core], old_d, aux_sem.at[8])]
    for copy in aux:
        copy.start()

    def add_into(out, *parts):
        total = parts[0][...].astype(F32)
        for part in parts[1:]:
            total = total + part[...].astype(F32)
        out[...] = total.astype(out.dtype)

    def x_first(j):
        return j % 2 == 0

    def first(j, i):
        kind, t, _, _ = MATRICES[j]
        group = (1 - x) * 2 + i if x_first(j) else i * 2 + (1 - y)
        return group, remote(own[kind].at[t, group], r1[kind].at[t, i], s1_s.at[j, i], s1_r.at[j, i], by_x if x_first(j) else by_y)

    def second(j):
        kind, t, _, _ = MATRICES[j]
        group, i = (x * 2 + (1 - y), 1 - y) if x_first(j) else ((1 - x) * 2 + y, 1 - x)
        return group, i, remote(own[kind].at[t, group], r2[kind].at[t], s2_s.at[j], s2_r.at[j], by_y if x_first(j) else by_x)

    def along(j, to, rightward):
        kind, t, _, _ = MATRICES[j]
        land, sems = (zl, zl_r) if rightward else (zr, zr_r)
        return remote(own[kind].at[t, chip[0], to], land[kind].at[t, to], z_s.at[j, to], sems.at[j, to], right if rightward else left)

    for j in SIX:
        kind, t, _, _ = MATRICES[j]
        to_partner(j).wait_recv()
        bring(j).wait()
        for i in range(2):
            group, copy = first(j, i)

            @pl.loop(0, 4)
            def _(b):
                add_into(own[kind].at[t, group, b], own[kind].at[t, group, b], two[kind].at[t, group, b])

            copy.start()
    for j in SIX:
        kind, t, _, _ = MATRICES[j]
        for i in range(2):
            first(j, i)[1].wait_recv()
        group, i, copy = second(j)

        @pl.loop(0, 4)
        def _(b):
            add_into(own[kind].at[t, group, b], own[kind].at[t, group, b], two[kind].at[t, group, b], r1[kind].at[t, i, b])

        copy.start()

    def partial(j, to):
        kind, t, _, _ = MATRICES[j]
        add_into(tmp[kind], own[kind].at[t, chip[0], to], two[kind].at[t, chip[0], to], r1[kind].at[t, y if x_first(j) else x, to], r2[kind].at[t, to])

    def add_landed(j, to, rightward):
        kind, t, _, _ = MATRICES[j]
        along(j, to, rightward).wait_recv()
        land = zl if rightward else zr
        add_into(tmp[kind], tmp[kind], land[kind].at[t, to])

    def pass_on(j, to, rightward):
        kind, t, _, _ = MATRICES[j]
        partial(j, to)

        @pl.when(z > 0 if rightward else z < 3)
        def _():
            add_landed(j, to, rightward)

        own[kind][t, chip[0], to] = tmp[kind][...].astype(BF16)
        along(j, to, rightward).start()

    squares = None
    for j in SIX:
        second(j)[2].wait_recv()
        for to in range(3):

            @pl.when(3 - to > z)
            def _():
                pass_on(j, 3 - to, True)

            @pl.when(to < z)
            def _():
                pass_on(j, to, False)

    for j in SIX:
        kind, t, _, _ = MATRICES[j]
        partial(j, z)

        @pl.when(z > 0)
        def _():
            add_landed(j, z, True)

        @pl.when(z < 3)
        def _():
            add_landed(j, z, False)

        total = tmp[kind][...].astype(BF16)
        if kind == "w":
            g_w[t, core] = total
            remote(g_w.at[t, core], g_w.at[t, core], g_s.at[t], g_r.at[t], partner).start()
        else:
            g_d[t] = total
        wide = total.astype(F32)
        for r in range(0, wide.shape[0], 8):
            for c in range(0, wide.shape[1], 128):
                part = wide[r : r + 8, c : c + 128]
                squares = part * part if squares is None else squares + part * part

    for j in SIX:
        to_partner(j).wait_send()
        for i in range(2):
            first(j, i)[1].wait_send()
        second(j)[2].wait_send()
        for to in range(4):

            @pl.when(to != z)
            def _():
                along(j, to, True).wait_send()

    norm[0] = squares
    for s, other in enumerate((partner, by_x, by_y)):
        copy = remote(norm.at[2 * s], norm.at[2 * s + 1], n_s.at[s], n_r.at[s], other)
        copy.start()
        copy.wait()
        norm[2 * s + 2] = norm[2 * s] + norm[2 * s + 1]
    norm[7 + z] = norm[6]
    for o in range(3):
        remote(norm.at[6], norm.at[7 + z], n_s.at[3 + o], nz_r.at[z], line[o]).start()
    for o in range(3):
        there = lax.rem(z + o + 1, 4)
        remote(norm.at[6], norm.at[7 + there], n_s.at[3 + o], nz_r.at[there], line[o]).wait()
    total = (norm[7] + norm[8]) + (norm[9] + norm[10])
    total = jnp.sum(jnp.sum(total, axis=1, keepdims=True), axis=0, keepdims=True)
    factor = jnp.minimum(1.0, 0.5 * lax.rsqrt(total / count + 1e-30))

    def update(w, m, v, g):
        g = g.astype(F32) * factor
        m = 0.9 * m + 0.1 * g
        v = 0.95 * v + 0.05 * g * g
        step = m * lax.rsqrt(v + 1e-8) + 0.1 * w.astype(F32)
        return (w.astype(F32) - 0.02 * step).astype(BF16), m, v

    for copy in aux:
        copy.wait()

    def swap(t):
        return remote(new_w.at[t, 1 - core], got_w.at[t], w_s.at[t], w_r.at[t], partner)

    for t in range(4):
        arg, layer = t % 2, 1 - t // 2
        theirs = remote(g_w.at[t, 1 - core], g_w.at[t, 1 - core], g_s.at[t], g_r.at[t], partner)
        theirs.wait_recv()
        for h in range(2):
            cut = slice(h * half, (h + 1) * half)
            w, m, v = update(old_w[arg, layer, :, cut], state_w[arg, layer, :, cut], state_w[2 + arg, layer, :, cut], g_w[t, h])
            new_w[t, h], state_w[arg, layer, :, cut], state_w[2 + arg, layer, :, cut] = w, m, v
        swap(t).start()
    for t in range(2):
        layer = 1 - t
        w, m, v = update(old_d[layer], state_d[0, layer], state_d[1, layer], g_d[t])
        own_d[t, chip[0], z], state_d[0, layer], state_d[1, layer] = w, m, v
    for t in range(4):
        swap(t).wait_recv()
        rows = lax.broadcasted_iota(jnp.int32, tmp_w.shape, 0)
        mine = (rows < tmp_w.shape[0] // 2) == (core == 0)
        own_w[t, chip[0], z] = jnp.where(mine, new_w[t, core].astype(F32), got_w[t].astype(F32)).astype(BF16)
    back = [pltpu.make_async_copy((state_w, state_w, state_w, state_w, state_d, state_d)[i].at[(0, 1, 2, 3, 0, 1)[i]], out_m[i], aux_sem.at[i]) for i in SIX]
    for copy in back:
        copy.start()

    def spread(j, group, zs, sem, to):
        kind, t, _, _ = MATRICES[j]
        place = own[kind].at[t, group, zs]
        return remote(place, place, sem, ag_r.at[j, group, zs], to)

    def near(j):
        return by_y if x_first(j) else by_x

    def far(j):
        return by_x if x_first(j) else by_y

    def groups(j):
        a, b = x * 2 + (1 - y), (1 - x) * 2 + y
        return (x * 2 + y, *((a, b) if x_first(j) else (b, a)), (1 - x) * 2 + (1 - y))

    def sideways(j, zs):
        spread(j, chip[0], zs, ag2_s.at[j, zs], far(j)).start()
        spread(j, chip[0], zs, ag1_s.at[j, zs], near(j)).start()

    def arrived(j, group, zs):
        spread(j, group, zs, ag1_s.at[j, zs], partner).wait_recv()

    def onward(j, zs):
        arrived(j, groups(j)[1], zs)
        spread(j, groups(j)[1], zs, ag3_s.at[j, zs], far(j)).start()

    for j in SIX:

        @pl.when(z < 3)
        def _():
            spread(j, chip[0], z, agz_s.at[j, z, 0], right).start()

        @pl.when(z > 0)
        def _():
            spread(j, chip[0], z, agz_s.at[j, z, 1], left).start()

        sideways(j, z)
    for d in (1, 2, 3, 4):
        for j in SIX:
            if d < 4:

                @pl.when(z - d >= 0)
                def _():
                    arrived(j, chip[0], z - d)

                    @pl.when(z < 3)
                    def _():
                        spread(j, chip[0], z - d, agz_s.at[j, z - d, 0], right).start()

                    sideways(j, z - d)

                @pl.when(z + d <= 3)
                def _():
                    arrived(j, chip[0], z + d)

                    @pl.when(z > 0)
                    def _():
                        spread(j, chip[0], z + d, agz_s.at[j, z + d, 1], left).start()

                    sideways(j, z + d)

            if d == 1:
                onward(j, z)
            else:

                @pl.when(z - (d - 1) >= 0)
                def _():
                    onward(j, z - (d - 1))

                @pl.when(z + (d - 1) <= 3)
                def _():
                    onward(j, z + (d - 1))

    def across(j, i):
        kind, t, _, _ = MATRICES[j]
        group = groups(j)[i]
        return group, remote(own[kind].at[t, group], two[kind].at[t, group], agt_s.at[j, i], agt_r.at[j, group], partner)

    def put(j, group, c, buffer, sem):
        kind, t, layer, arg = MATRICES[j]
        to = out_w[arg].at[layer, group, :, :, columns(c)] if kind == "w" else out_w[arg].at[layer, group, :, c]
        return pltpu.make_async_copy(buffer[kind].at[t, group], to, sem)

    for i in range(4):
        for j in SIX:
            if i >= 2:
                for zs in range(4):
                    arrived(j, groups(j)[i], zs)
            group, copy = across(j, i)
            copy.start()
            put(j, group, core, own, out_s.at[j, i]).start()
        if i:
            for j in SIX:
                group, copy = across(j, i - 1)
                copy.wait_recv()
                put(j, group, 1 - core, two, out2_s.at[j, i - 1]).start()
    for j in SIX:
        group, copy = across(j, 3)
        copy.wait_recv()
        put(j, group, 1 - core, two, out2_s.at[j, 3]).start()

    for copy in back:
        copy.wait()
    for t in range(4):
        remote(g_w.at[t, core], g_w.at[t, core], g_s.at[t], g_r.at[t], partner).wait_send()
        swap(t).wait_send()
    for j in SIX:
        for zs in range(4):
            spread(j, chip[0], zs, ag1_s.at[j, zs], near(j)).wait_send()
            spread(j, chip[0], zs, ag2_s.at[j, zs], far(j)).wait_send()
            spread(j, chip[0], zs, ag3_s.at[j, zs], far(j)).wait_send()

            @pl.when(jnp.logical_and(zs <= z, z < 3))
            def _():
                spread(j, chip[0], zs, agz_s.at[j, zs, 0], right).wait_send()

            @pl.when(jnp.logical_and(zs >= z, z > 0))
            def _():
                spread(j, chip[0], zs, agz_s.at[j, zs, 1], left).wait_send()

        for i in range(4):
            group, copy = across(j, i)
            copy.wait_send()
            put(j, group, core, own, out_s.at[j, i]).wait()
            put(j, group, 1 - core, two, out2_s.at[j, i]).wait()


def reduce_step_gather(terms, weights, moments):
    wide = next(t for t, m in zip(terms, MATRICES) if m[0] == "w").shape
    down = terms[0].shape
    rw, cw, rd, cd = wide[2], wide[3] // 2, down[3], down[4]
    count = 4 * 16 * rw * 2 * cw + 2 * 32 * rd * cd
    vm, dma = pltpu.VMEM, pltpu.SemaphoreType.DMA
    w, d = (rw, cw), (rd, cd)
    scratch = [
        vm((4, 4, 4, *w), BF16), vm((2, 4, 4, *d), BF16), vm((4, 4, 4, *w), BF16), vm((2, 4, 4, *d), BF16),
        vm((4, 2, 4, *w), BF16), vm((2, 2, 4, *d), BF16), vm((4, 4, *w), BF16), vm((2, 4, *d), BF16),
        vm((4, 4, *w), BF16), vm((2, 4, *d), BF16), vm((4, 4, *w), BF16), vm((2, 4, *d), BF16),
        vm(w, F32), vm(d, F32), vm((4, 2, *w), BF16), vm((2, *d), BF16),
        vm((4, 2, rw, 2 * cw), F32), vm((2, 2, *d), F32), vm((2, 2, rw, 2 * cw), BF16), vm((2, *d), BF16),
        vm((4, 2, *w), BF16), vm((4, *w), BF16), vm((11, 8, 128), F32),
        dma((6,)), dma((9,)), dma((6,)), dma((6,)), dma((6, 2)), dma((6, 2)), dma((6,)), dma((6,)), dma((6, 4)), dma((6, 4)), dma((6, 4)),
        dma((4,)), dma((4,)), dma((6,)), dma((3,)), dma((4,)), dma((4,)), dma((4,)),
        dma((6, 4, 4)), dma((6, 4, 2)), dma((6, 4)), dma((6, 4)), dma((6, 4)), dma((6, 4)), dma((6, 4)), dma((6, 4)), dma((6, 4)),
    ]
    outs = [jax.ShapeDtypeStruct(a.shape, a.dtype) for a in (*weights, *moments)]
    return pl.pallas_call(
        functools.partial(step_kernel, count),
        out_shape=outs,
        in_specs=[pl.BlockSpec(memory_space=pl.ANY)] * 15,
        out_specs=[pl.BlockSpec(memory_space=pl.ANY)] * 9,
        scratch_shapes=scratch,
        compiler_params=pltpu.CompilerParams(collective_id=0, has_side_effects=True, vmem_limit_bytes=60 * 2**20),
        name="reduce_step_gather",
    )(*terms, *weights, *moments)


def all_steps(me, terms, w, m, v):
    core = me % 2

    def blocks(t):
        return t.reshape(*t.shape[:-2], 4, 4, t.shape[-2] // 16, t.shape[-1])

    def down_blocks(t):
        return t.reshape(*t.shape[:-2], 4, 4, 2, t.shape[-2] // 32, t.shape[-1])

    ordered = [(blocks if kind == "w" else down_blocks)(terms[layer][arg]) for kind, _, layer, arg in MATRICES]
    twice = [jnp.concatenate([t, t], axis=1) for t in (m[0], m[1], v[0], v[1])]
    weights = [blocks(w[0]), blocks(w[1]), down_blocks(w[2])]
    out = reduce_step_gather(ordered, weights, [*twice, m[2], v[2]])
    new = [a.reshape(b.shape) for a, b in zip(out[:3], w)]
    rows = m[0].shape[1]
    mine = [jnp.where(core == 0, t[:, :rows], t[:, rows:]) for t in out[3:7]]
    return (*new, mine[0], mine[1], out[7], mine[2], mine[3], out[8])


def solution(mesh):
    def body(x, dy, *arrays):
        w, m, v = (arrays[i : i + 3] for i in (0, 3, 6))
        return all_steps(lax.axis_index("dp"), gradients(x[0], dy[0], *w), w, m, v)

    moments = P(None, "dp", None)
    return jax.shard_map(
        body,
        mesh=mesh,
        in_specs=(P(("rep", "dp")), P(("rep", "dp")), *[P()] * 3, *[moments] * 6),
        out_specs=(*[P("rep")] * 3, *[P("rep", "dp")] * 6),
        check_vma=False,
    )
```

```python
import functools

import jax
import jax.numpy as jnp
from jax import lax
from jax.experimental import pallas as pl
from jax.experimental.pallas import tpu as pltpu
from jax.sharding import PartitionSpec as P

F32, BF16 = jnp.float32, jnp.bfloat16


def dot(a, b, ca, cb):
    return lax.dot_general(a, b, (((ca,), (cb,)), ((), ())), preferred_element_type=F32)


def states_kernel(x_ref, dy_ref, wg_hbm, wu_hbm, wd_hbm, a1t, a2t, dh1t, dyt, s1, s2, dg1, du1, dg2, du2, wg, wu, wd, silu1, slope1, sems):
    width = min(512, wg.shape[2])
    cuts = [slice(i, i + width) for i in range(0, wg.shape[2], width)]
    first = pl.program_id(0) == 0
    order = [(wg_hbm, wg, 0), (wu_hbm, wu, 0), (wd_hbm, wd, 0), (wg_hbm, wg, 1), (wu_hbm, wu, 1), (wd_hbm, wd, 1)]
    copies = [pltpu.make_async_copy(src.at[layer], dst.at[layer], sems.at[i]) for i, (src, dst, layer) in enumerate(order)]

    @pl.when(first)
    def _():
        for copy in copies:
            copy.start()

    def need(*which):
        @pl.when(first)
        def _():
            for i in which:
                copies[i].wait()

    def normed(h):
        wide = h.astype(F32)
        r = lax.rsqrt(jnp.mean(wide * wide, -1, keepdims=True) + 1e-6)
        return wide, r, (wide * r).astype(BF16)

    def gated(a, layer, cut):
        gate, up = dot(a, wg[layer, :, cut], 1, 0), dot(a, wu[layer, :, cut], 1, 0)
        sig = 0.5 * jnp.tanh(0.5 * gate) + 0.5
        silu = gate * sig
        return silu, up * (sig + silu * (1 - sig)), (silu * up).astype(BF16)

    def hidden_back(d, layer, cut, silu, slope):
        ds = dot(d, wd[layer, cut, :], 1, 1).astype(BF16).astype(F32)
        return (ds * slope).astype(BF16), (ds * silu).astype(BF16)

    h0, dy = x_ref[...], dy_ref[...]
    _, _, a1 = normed(h0)
    need(0, 1)
    for cut in cuts:
        silu1[:, cut], slope1[:, cut], s1[:, cut] = gated(a1, 0, cut)
    a1t[...] = a1.T
    dyt[...] = dy.T
    need(2)
    h1 = (h0.astype(F32) + dot(s1[...], wd[0], 1, 0).astype(BF16).astype(F32)).astype(BF16)
    wide1, r1, a2 = normed(h1)
    need(3, 4, 5)
    for cut in cuts:
        silu, slope, s2[:, cut] = gated(a2, 1, cut)
        dg2[:, cut], du2[:, cut] = hidden_back(dy, 1, cut, silu, slope)
    a2t[...] = a2.T
    by_gate, by_up = (dot(d[...], w[1], 1, 1).astype(BF16).astype(F32) for d, w in ((dg2, wg), (du2, wu)))
    da2 = (by_gate + by_up).astype(BF16).astype(F32)
    back = da2 * r1 - wide1 * (r1 * r1 * r1 * jnp.mean(da2 * wide1, -1, keepdims=True))
    dh1 = (dy.astype(F32) + back.astype(BF16).astype(F32)).astype(BF16)
    for cut in cuts:
        dg1[:, cut], du1[:, cut] = hidden_back(dh1, 0, cut, silu1[:, cut], slope1[:, cut])
    dh1t[...] = dh1.T


def states(x, dy, wg, wu, wd):
    (tokens, d), ff = x.shape, wg.shape[2]
    block = min(256, tokens)
    rows = pl.BlockSpec((block, d), lambda i: (i, 0))
    flipped = pl.BlockSpec((d, block), lambda i: (0, i))
    hidden = pl.BlockSpec((block, ff), lambda i: (i, 0))
    return pl.pallas_call(
        states_kernel,
        grid=(tokens // block,),
        out_shape=[jax.ShapeDtypeStruct((d, tokens), BF16)] * 4 + [jax.ShapeDtypeStruct((tokens, ff), BF16)] * 6,
        in_specs=[rows, rows] + [pl.BlockSpec(memory_space=pl.ANY)] * 3,
        out_specs=[flipped] * 4 + [hidden] * 6,
        scratch_shapes=[pltpu.VMEM(w.shape, BF16) for w in (wg, wu, wd)]
        + [pltpu.VMEM((block, ff), F32)] * 2
        + [pltpu.SemaphoreType.DMA((6,))],
        compiler_params=pltpu.CompilerParams(vmem_limit_bytes=60 * 2**20),
        name="states",
    )(x, dy, wg, wu, wd)


MESH = pl.DeviceIdType.MESH
MATRICES = (("d", 0, 1, 2), ("w", 0, 1, 0), ("w", 1, 1, 1), ("d", 1, 0, 2), ("w", 2, 0, 0), ("w", 3, 0, 1))
SIX = range(6)
LEFT = (0, 1, 1, 2, 3, 3)


def step_kernel(count, *refs):
    lefts, rights, weights, moments, out_w, out_m = refs[0:4], refs[4:10], refs[10:13], refs[13:19], refs[19:22], refs[22:28]
    own_w, own_d, two_w, two_d, r1_w, r1_d, r2_w, r2_d, zl_w, zl_d, zr_w, zr_d = refs[28:40]
    tmp_w, tmp_d, g_w, g_d, state_w, state_d, old_w, old_d, new_w, got_w, norm = refs[40:51]
    (loc_sem, aux_sem, two_s, two_r, s1_s, s1_r, s2_s, s2_r, z_s, zl_r, zr_r, g_s, g_r, n_s, n_r, nz_r, w_s, w_r, ag_r, agz_s, ag1_s, ag2_s,
     ag3_s, agt_s, agt_r, out_s, out2_s) = refs[51:78]
    left_v, right_v, stage_w, stage_d, left_sem, right_sem = refs[78:84]
    own, two = {"w": own_w, "d": own_d}, {"w": two_w, "d": two_d}
    r1, r2 = {"w": r1_w, "d": r1_d}, {"w": r2_w, "d": r2_d}
    zl, zr, tmp = {"w": zl_w, "d": zl_d}, {"w": zr_w, "d": zr_d}, {"w": tmp_w, "d": tmp_d}

    me = lax.axis_index("dp")
    core, z, y, x = lax.rem(me, 2), lax.rem(me // 2, 4), lax.rem(me // 8, 2), me // 16
    half = own_w.shape[-1]

    def device(x, y, z, core):
        return {"dp": ((x * 2 + y) * 4 + z) * 2 + core}

    partner = device(x, y, z, 1 - core)
    by_x, by_y = device(1 - x, y, z, core), device(x, 1 - y, z, core)
    right, left = device(x, y, z + 1, core), device(x, y, z - 1, core)
    line = [device(x, y, lax.rem(z + o, 4), core) for o in (1, 2, 3)]

    def columns(c):
        return pl.ds(pl.multiple_of(c * half, 128), half)

    def remote(src, dst, send, recv, to):
        return pltpu.make_async_remote_copy(src_ref=src, dst_ref=dst, send_sem=send, recv_sem=recv, device_id=to, device_id_type=MESH)

    barrier = pltpu.get_barrier_semaphore()
    for other in (partner, by_x, by_y, *line):
        pl.semaphore_signal(barrier, inc=1, device_id=other, device_id_type=MESH)
    pl.semaphore_wait(barrier, 6)

    def to_partner(j):
        kind, t, _, _ = MATRICES[j]
        return remote(stage_w.at[t % 2] if kind == "w" else stage_d, two[kind].at[t], two_s.at[j], two_r.at[j], partner)

    def left_copy(i):
        return pltpu.make_async_copy(lefts[i], left_v.at[i % 2], left_sem.at[i])

    def right_copy(n):
        j, part = n // 2, n % 2
        if MATRICES[j][0] == "w":
            part = core if part else 1 - core
        size = right_v.shape[2]
        return pltpu.make_async_copy(rights[j].at[:, pl.ds(pl.multiple_of(part * size, 128), size)], right_v.at[n % 2], right_sem.at[n])

    def make(j):
        kind, t, _, _ = MATRICES[j]
        factor_l = left_v.at[LEFT[j] % 2]
        if j == 0 or LEFT[j] != LEFT[j - 1]:
            left_copy(LEFT[j]).wait()
        if kind == "w" and t >= 2:
            to_partner(j - 3).wait_send()
        if kind == "d" and t:
            to_partner(j - 3).wait_send()
        for part in range(2):
            n = 2 * j + part
            right_copy(n).wait()
            factor_r = right_v.at[n % 2]
            if kind == "w":
                width = min(256, half)

                @pl.loop(0, half // width)
                def _(q):
                    cut = pl.ds(pl.multiple_of(q * width, width), width)
                    made = dot(factor_l[...], factor_r[:, cut], 1, 0).astype(BF16)
                    made = made.reshape(4, 4, own_w.shape[3], width)
                    if part:
                        own_w[t, :, :, :, cut] = made
                    else:
                        stage_w[t % 2, :, :, :, cut] = made

                if part == 0:
                    to_partner(j).start()
            else:
                width = factor_r.shape[1] // 2

                @pl.loop(0, 2)
                def _(q):
                    made = dot(factor_l[...], factor_r[:, pl.ds(pl.multiple_of(q * width, width), width)], 1, 0).T
                    made = made.reshape(4, 2, *own_d.shape[3:])
                    own_d[t, part * 2 + q] = jnp.where(core == 0, made[:, 0], made[:, 1]).astype(BF16)
                    stage_d[part * 2 + q] = jnp.where(core == 0, made[:, 1], made[:, 0]).astype(BF16)

                if part:
                    to_partner(j).start()
            if n + 2 < 12:
                right_copy(n + 2).start()
        if j in (0, 2):
            left_copy(LEFT[j] + 2).start()

    for i in range(2):
        left_copy(i).start()
        right_copy(i).start()
    chip = (x * 2 + y, z)
    aux = [pltpu.make_async_copy(moments[i], (state_w, state_w, state_w, state_w, state_d, state_d)[i].at[(0, 1, 2, 3, 0, 1)[i]], aux_sem.at[i]) for i in SIX]
    aux += [pltpu.make_async_copy(weights[i].at[:, chip[0], chip[1]], old_w.at[i], aux_sem.at[6 + i]) for i in range(2)]
    aux += [pltpu.make_async_copy(weights[2].at[:, chip[0], chip[1], core], old_d, aux_sem.at[8])]
    for copy in aux:
        copy.start()

    def add_into(out, *parts):
        total = parts[0][...].astype(F32)
        for part in parts[1:]:
            total = total + part[...].astype(F32)
        out[...] = total.astype(out.dtype)

    def x_first(j):
        return j % 2 == 0

    def first(j, i):
        kind, t, _, _ = MATRICES[j]
        group = (1 - x) * 2 + i if x_first(j) else i * 2 + (1 - y)
        return group, remote(own[kind].at[t, group], r1[kind].at[t, i], s1_s.at[j, i], s1_r.at[j, i], by_x if x_first(j) else by_y)

    def second(j):
        kind, t, _, _ = MATRICES[j]
        group, i = (x * 2 + (1 - y), 1 - y) if x_first(j) else ((1 - x) * 2 + y, 1 - x)
        return group, i, remote(own[kind].at[t, group], r2[kind].at[t], s2_s.at[j], s2_r.at[j], by_y if x_first(j) else by_x)

    def along(j, to, rightward):
        kind, t, _, _ = MATRICES[j]
        land, sems = (zl, zl_r) if rightward else (zr, zr_r)
        return remote(own[kind].at[t, chip[0], to], land[kind].at[t, to], z_s.at[j, to], sems.at[j, to], right if rightward else left)

    def leave_first(j):
        kind, t, _, _ = MATRICES[j]
        to_partner(j).wait_recv()
        for i in range(2):
            group, copy = first(j, i)

            @pl.loop(0, 4)
            def _(b):
                add_into(own[kind].at[t, group, b], own[kind].at[t, group, b], two[kind].at[t, group, b])

            copy.start()

    def leave_second(j):
        kind, t, _, _ = MATRICES[j]
        for i in range(2):
            first(j, i)[1].wait_recv()
        group, i, copy = second(j)

        @pl.loop(0, 4)
        def _(b):
            add_into(own[kind].at[t, group, b], own[kind].at[t, group, b], two[kind].at[t, group, b], r1[kind].at[t, i, b])

        copy.start()

    for j in SIX:
        make(j)
        leave_first(j)
        if j >= 3:
            leave_second(j - 3)
    for j in (3, 4, 5):
        leave_second(j)

    def partial(j, to):
        kind, t, _, _ = MATRICES[j]
        add_into(tmp[kind], own[kind].at[t, chip[0], to], two[kind].at[t, chip[0], to], r1[kind].at[t, y if x_first(j) else x, to], r2[kind].at[t, to])

    def add_landed(j, to, rightward):
        kind, t, _, _ = MATRICES[j]
        along(j, to, rightward).wait_recv()
        land = zl if rightward else zr
        add_into(tmp[kind], tmp[kind], land[kind].at[t, to])

    def pass_on(j, to, rightward):
        kind, t, _, _ = MATRICES[j]
        partial(j, to)

        @pl.when(z > 0 if rightward else z < 3)
        def _():
            add_landed(j, to, rightward)

        own[kind][t, chip[0], to] = tmp[kind][...].astype(BF16)
        along(j, to, rightward).start()

    squares = None
    for j in SIX:
        second(j)[2].wait_recv()
        for to in range(3):

            @pl.when(3 - to > z)
            def _():
                pass_on(j, 3 - to, True)

            @pl.when(to < z)
            def _():
                pass_on(j, to, False)

    for j in SIX:
        kind, t, _, _ = MATRICES[j]
        partial(j, z)

        @pl.when(z > 0)
        def _():
            add_landed(j, z, True)

        @pl.when(z < 3)
        def _():
            add_landed(j, z, False)

        total = tmp[kind][...].astype(BF16)
        if kind == "w":
            g_w[t, core] = total
            remote(g_w.at[t, core], g_w.at[t, core], g_s.at[t], g_r.at[t], partner).start()
        else:
            g_d[t] = total
        wide = total.astype(F32)
        for r in range(0, wide.shape[0], 8):
            for c in range(0, wide.shape[1], 128):
                part = wide[r : r + 8, c : c + 128]
                squares = part * part if squares is None else squares + part * part

    for j in SIX:
        if j >= 3:
            to_partner(j).wait_send()
        for i in range(2):
            first(j, i)[1].wait_send()
        second(j)[2].wait_send()
        for to in range(4):

            @pl.when(to != z)
            def _():
                along(j, to, True).wait_send()

    norm[0] = squares
    for s, other in enumerate((partner, by_x, by_y)):
        copy = remote(norm.at[2 * s], norm.at[2 * s + 1], n_s.at[s], n_r.at[s], other)
        copy.start()
        copy.wait()
        norm[2 * s + 2] = norm[2 * s] + norm[2 * s + 1]
    norm[7 + z] = norm[6]
    for o in range(3):
        remote(norm.at[6], norm.at[7 + z], n_s.at[3 + o], nz_r.at[z], line[o]).start()
    for o in range(3):
        there = lax.rem(z + o + 1, 4)
        remote(norm.at[6], norm.at[7 + there], n_s.at[3 + o], nz_r.at[there], line[o]).wait()
    total = (norm[7] + norm[8]) + (norm[9] + norm[10])
    total = jnp.sum(jnp.sum(total, axis=1, keepdims=True), axis=0, keepdims=True)
    factor = jnp.minimum(1.0, 0.5 * lax.rsqrt(total / count + 1e-30))

    def update(w, m, v, g):
        g = g.astype(F32) * factor
        m = 0.9 * m + 0.1 * g
        v = 0.95 * v + 0.05 * g * g
        step = m * lax.rsqrt(v + 1e-8) + 0.1 * w.astype(F32)
        return (w.astype(F32) - 0.02 * step).astype(BF16), m, v

    for copy in aux:
        copy.wait()

    def swap(t):
        return remote(new_w.at[t, 1 - core], got_w.at[t], w_s.at[t], w_r.at[t], partner)

    for t in range(4):
        arg, layer = t % 2, 1 - t // 2
        theirs = remote(g_w.at[t, 1 - core], g_w.at[t, 1 - core], g_s.at[t], g_r.at[t], partner)
        theirs.wait_recv()
        for h in range(2):
            cut = slice(h * half, (h + 1) * half)
            w, m, v = update(old_w[arg, layer, :, cut], state_w[arg, layer, :, cut], state_w[2 + arg, layer, :, cut], g_w[t, h])
            new_w[t, h], state_w[arg, layer, :, cut], state_w[2 + arg, layer, :, cut] = w, m, v
        swap(t).start()
    for t in range(2):
        layer = 1 - t
        w, m, v = update(old_d[layer], state_d[0, layer], state_d[1, layer], g_d[t])
        own_d[t, chip[0], z], state_d[0, layer], state_d[1, layer] = w, m, v
    for t in range(4):
        swap(t).wait_recv()
        rows = lax.broadcasted_iota(jnp.int32, tmp_w.shape, 0)
        mine = (rows < tmp_w.shape[0] // 2) == (core == 0)
        own_w[t, chip[0], z] = jnp.where(mine, new_w[t, core].astype(F32), got_w[t].astype(F32)).astype(BF16)
    back = [pltpu.make_async_copy((state_w, state_w, state_w, state_w, state_d, state_d)[i].at[(0, 1, 2, 3, 0, 1)[i]], out_m[i], aux_sem.at[i]) for i in SIX]
    for copy in back:
        copy.start()

    def spread(j, group, zs, sem, to):
        kind, t, _, _ = MATRICES[j]
        place = own[kind].at[t, group, zs]
        return remote(place, place, sem, ag_r.at[j, group, zs], to)

    def near(j):
        return by_y if x_first(j) else by_x

    def far(j):
        return by_x if x_first(j) else by_y

    def groups(j):
        a, b = x * 2 + (1 - y), (1 - x) * 2 + y
        return (x * 2 + y, *((a, b) if x_first(j) else (b, a)), (1 - x) * 2 + (1 - y))

    def sideways(j, zs):
        spread(j, chip[0], zs, ag2_s.at[j, zs], far(j)).start()
        spread(j, chip[0], zs, ag1_s.at[j, zs], near(j)).start()

    def arrived(j, group, zs):
        spread(j, group, zs, ag1_s.at[j, zs], partner).wait_recv()

    def onward(j, zs):
        arrived(j, groups(j)[1], zs)
        spread(j, groups(j)[1], zs, ag3_s.at[j, zs], far(j)).start()

    for j in SIX:

        @pl.when(z < 3)
        def _():
            spread(j, chip[0], z, agz_s.at[j, z, 0], right).start()

        @pl.when(z > 0)
        def _():
            spread(j, chip[0], z, agz_s.at[j, z, 1], left).start()

        sideways(j, z)
    for d in (1, 2, 3, 4):
        for j in SIX:
            if d < 4:

                @pl.when(z - d >= 0)
                def _():
                    arrived(j, chip[0], z - d)

                    @pl.when(z < 3)
                    def _():
                        spread(j, chip[0], z - d, agz_s.at[j, z - d, 0], right).start()

                    sideways(j, z - d)

                @pl.when(z + d <= 3)
                def _():
                    arrived(j, chip[0], z + d)

                    @pl.when(z > 0)
                    def _():
                        spread(j, chip[0], z + d, agz_s.at[j, z + d, 1], left).start()

                    sideways(j, z + d)

            if d == 1:
                onward(j, z)
            else:

                @pl.when(z - (d - 1) >= 0)
                def _():
                    onward(j, z - (d - 1))

                @pl.when(z + (d - 1) <= 3)
                def _():
                    onward(j, z + (d - 1))

    def across(j, i):
        kind, t, _, _ = MATRICES[j]
        group = groups(j)[i]
        return group, remote(own[kind].at[t, group], two[kind].at[t, group], agt_s.at[j, i], agt_r.at[j, group], partner)

    def put(j, group, c, buffer, sem):
        kind, t, layer, arg = MATRICES[j]
        to = out_w[arg].at[layer, group, :, :, columns(c)] if kind == "w" else out_w[arg].at[layer, group, :, c]
        return pltpu.make_async_copy(buffer[kind].at[t, group], to, sem)

    for i in range(4):
        for j in SIX:
            if i >= 2:
                for zs in range(4):
                    arrived(j, groups(j)[i], zs)
            group, copy = across(j, i)
            copy.start()
            put(j, group, core, own, out_s.at[j, i]).start()
        if i:
            for j in SIX:
                group, copy = across(j, i - 1)
                copy.wait_recv()
                put(j, group, 1 - core, two, out2_s.at[j, i - 1]).start()
    for j in SIX:
        group, copy = across(j, 3)
        copy.wait_recv()
        put(j, group, 1 - core, two, out2_s.at[j, 3]).start()

    for copy in back:
        copy.wait()
    for t in range(4):
        remote(g_w.at[t, core], g_w.at[t, core], g_s.at[t], g_r.at[t], partner).wait_send()
        swap(t).wait_send()
    for j in SIX:
        for zs in range(4):
            spread(j, chip[0], zs, ag1_s.at[j, zs], near(j)).wait_send()
            spread(j, chip[0], zs, ag2_s.at[j, zs], far(j)).wait_send()
            spread(j, chip[0], zs, ag3_s.at[j, zs], far(j)).wait_send()

            @pl.when(jnp.logical_and(zs <= z, z < 3))
            def _():
                spread(j, chip[0], zs, agz_s.at[j, zs, 0], right).wait_send()

            @pl.when(jnp.logical_and(zs >= z, z > 0))
            def _():
                spread(j, chip[0], zs, agz_s.at[j, zs, 1], left).wait_send()

        for i in range(4):
            group, copy = across(j, i)
            copy.wait_send()
            put(j, group, core, own, out_s.at[j, i]).wait()
            put(j, group, 1 - core, two, out2_s.at[j, i]).wait()


def reduce_step_gather(lefts, rights, weights, moments):
    (d_model, tokens), ff = lefts[0].shape, rights[0].shape[1]
    rw, cw, rd, cd = d_model // 16, ff // 2, ff // 32, d_model
    count = 4 * 16 * rw * 2 * cw + 2 * 32 * rd * cd
    vm, dma = pltpu.VMEM, pltpu.SemaphoreType.DMA
    w, d = (rw, cw), (rd, cd)
    scratch = [
        vm((4, 4, 4, *w), BF16), vm((2, 4, 4, *d), BF16), vm((4, 4, 4, *w), BF16), vm((2, 4, 4, *d), BF16),
        vm((4, 2, 4, *w), BF16), vm((2, 2, 4, *d), BF16), vm((4, 4, *w), BF16), vm((2, 4, *d), BF16),
        vm((4, 4, *w), BF16), vm((2, 4, *d), BF16), vm((4, 4, *w), BF16), vm((2, 4, *d), BF16),
        vm(w, F32), vm(d, F32), vm((4, 2, *w), BF16), vm((2, *d), BF16),
        vm((4, 2, rw, 2 * cw), F32), vm((2, 2, *d), F32), vm((2, 2, rw, 2 * cw), BF16), vm((2, *d), BF16),
        vm((4, 2, *w), BF16), vm((4, *w), BF16), vm((11, 8, 128), F32),
        dma((6,)), dma((9,)), dma((6,)), dma((6,)), dma((6, 2)), dma((6, 2)), dma((6,)), dma((6,)), dma((6, 4)), dma((6, 4)), dma((6, 4)),
        dma((4,)), dma((4,)), dma((6,)), dma((3,)), dma((4,)), dma((4,)), dma((4,)),
        dma((6, 4, 4)), dma((6, 4, 2)), dma((6, 4)), dma((6, 4)), dma((6, 4)), dma((6, 4)), dma((6, 4)), dma((6, 4)), dma((6, 4)),
        vm((2, d_model, tokens), BF16), vm((2, tokens, ff // 2), BF16), vm((2, 4, 4, *w), BF16), vm((4, 4, *d), BF16), dma((4,)), dma((12,)),
    ]
    outs = [jax.ShapeDtypeStruct(a.shape, a.dtype) for a in (*weights, *moments)]
    return pl.pallas_call(
        functools.partial(step_kernel, count),
        out_shape=outs,
        in_specs=[pl.BlockSpec(memory_space=pl.ANY)] * 19,
        out_specs=[pl.BlockSpec(memory_space=pl.ANY)] * 9,
        scratch_shapes=scratch,
        compiler_params=pltpu.CompilerParams(collective_id=0, has_side_effects=True, vmem_limit_bytes=67043328),
        name="reduce_step_gather",
    )(*lefts, *rights, *weights, *moments)


def all_steps(me, lefts, rights, w, m, v):
    core = me % 2

    def blocks(t):
        return t.reshape(*t.shape[:-2], 4, 4, t.shape[-2] // 16, t.shape[-1])

    def down_blocks(t):
        return t.reshape(*t.shape[:-2], 4, 4, 2, t.shape[-2] // 32, t.shape[-1])

    twice = [jnp.concatenate([t, t], axis=1) for t in (m[0], m[1], v[0], v[1])]
    weights = [blocks(w[0]), blocks(w[1]), down_blocks(w[2])]
    out = reduce_step_gather(lefts, rights, weights, [*twice, m[2], v[2]])
    new = [a.reshape(b.shape) for a, b in zip(out[:3], w)]
    rows = m[0].shape[1]
    mine = [jnp.where(core == 0, t[:, :rows], t[:, rows:]) for t in out[3:7]]
    return (*new, mine[0], mine[1], out[7], mine[2], mine[3], out[8])


def solution(mesh):
    def body(x, dy, *arrays):
        w, m, v = (arrays[i : i + 3] for i in (0, 3, 6))
        a1t, a2t, dh1t, dyt, s1, s2, dg1, du1, dg2, du2 = states(x[0], dy[0], *w)
        return all_steps(lax.axis_index("dp"), (dyt, a2t, dh1t, a1t), (s2, dg2, du2, s1, dg1, du1), w, m, v)

    moments = P(None, "dp", None)
    return jax.shard_map(
        body,
        mesh=mesh,
        in_specs=(P(("rep", "dp")), P(("rep", "dp")), *[P()] * 3, *[moments] * 6),
        out_specs=(*[P("rep")] * 3, *[P("rep", "dp")] * 6),
        check_vma=False,
    )
```
